512 devices in a mesh: groups: 2 (over y), tmpl: 128 (over z, x), det: 2 (over core).
Axes of the slice: x: 8, y: 2, z: 16, core: 2. Of those that a mesh axis runs over, the one named last changes fastest.
The devices are a block of a 8x8x16 slice.
Arguments:
- basis_series: bfloat16 [3, 128, 524288], P(None, None, ('groups', 'tmpl', 'det')), parts along dimension 2, may hold values from -6 to 6
- reconstruction: bfloat16 [3, 4096, 2, 128], P(None, ('groups', 'tmpl')), parts along dimension 1, may hold values from -0.5 to 0.5
- offsets: int32 [6], P('groups'), parts along dimension 0, may hold values from 1024 to 16383
Outputs:
- window_peaks: float32 [2048, 4096], P(None, ('groups', 'tmpl', 'det')), parts along dimension 1
The draws below stay inside these ranges and needn't reach their ends.
There are 2 independent parts, one for each index of `groups`. The reference program is written for one: setup_inputs(seed, part) draws one part's arguments, and reference() takes and returns one part's arrays. A program takes and returns all parts, laid end to end along the dimension named above; each array names one. Nothing has to cross between parts.
Inputs may be any that keep to these rules, and one draw needn't show every extreme that they name: `offsets`: slides are applied circularly over the segment's 262144 samples.
All inputs are finite; a program needn't handle non-finite values.
Results may differ from the reference program's by a relative error of at most 0.0003.
Values may be sent and summed in bfloat16 or wider, within the bound.
No kernel may reach another device: no remote copies, remote signals or barrier semaphores. Data moves between devices by JAX's collectives and lax.ppermute only.
A program may use at most 64 MiB of HBM per device.

```python
import jax
import jax.numpy as jnp
from jax import lax

DETS = 3
BASIS = 128
WIN = 128
T_DEV = 1024
MAXQ = 16
TEMPL = 2048
NT = 262144
NWIN = 2048


def level_of(key, dims, pieces, low, top_value):
    factor_of = 1.0
    for axis_at, shards_of in pieces:
        steps = jax.random.uniform(jax.random.fold_in(jax.random.fold_in(key, 6), axis_at), (shards_of,), jnp.float32, low / len(pieces), top_value / len(pieces))
        factor_of = factor_of * jnp.repeat(jnp.exp(steps), dims[axis_at] // shards_of).reshape((-1,) + (1,) * (len(dims) - 1 - axis_at))
    return factor_of


def bell_draw(key, shape, spread, limit, pieces=(), dtype=jnp.bfloat16):
    level = level_of(key, shape, pieces, -0.22, 0.18) if pieces else 1.0
    drawn = jax.random.normal(key, shape, jnp.float32) * spread * level
    return jnp.minimum(jnp.maximum(drawn, -limit), limit).astype(dtype)


def setup_inputs(seed: int = 0, part: int = 0) -> dict:
    key_of = jax.random.split(jax.random.key(seed), 4)
    part_keys = jax.random.split(jax.random.fold_in(key_of[3], part), 4)
    basis_series = bell_draw(part_keys[0], (DETS, BASIS, NT), 1.0, 6.0, ((2, 256),))
    reconstruction = bell_draw(part_keys[1], (DETS, TEMPL, 2, BASIS), BASIS ** -0.5, 0.5, ((1, 128),))
    offsets = jax.random.randint(part_keys[2], (DETS,), T_DEV, MAXQ * T_DEV).astype(jnp.int32)
    return dict(basis_series=basis_series, reconstruction=reconstruction, offsets=offsets)


def reference(basis_series, reconstruction, offsets):
    slid_series = jnp.stack([jnp.roll(basis_series[detector], -offsets[detector], axis=1) for detector in range(DETS)])
    block_count = NT // T_DEV
    blocks = slid_series.reshape(DETS, BASIS, block_count, T_DEV).transpose(2, 0, 1, 3)

    def one_block(block):
        power_sum = jnp.zeros((TEMPL, T_DEV), jnp.float32)
        for detector in range(DETS):
            filtered = jnp.dot(reconstruction[detector].reshape(2 * TEMPL, BASIS), block[detector], preferred_element_type=jnp.float32)
            filtered = filtered.reshape(TEMPL, 2, T_DEV)
            power_sum = power_sum + lax.optimization_barrier(jnp.sum(filtered * filtered, axis=1))
        network = jnp.sqrt(power_sum)
        return lax.optimization_barrier(jnp.max(network.reshape(TEMPL, T_DEV // WIN, WIN), axis=2))
    peaks = lax.map(one_block, blocks)
    return peaks.transpose(1, 0, 2).reshape(TEMPL, NWIN)
```

```python
import functools
import math

import jax
import jax.numpy as jnp
from jax import lax
from jax.experimental import pallas as pl
from jax.experimental.pallas import tpu as pltpu
from jax.sharding import PartitionSpec as P

DETS = 3
WIN = 128
SLIDES = 16
ROW = 8
BOTH = ("tmpl", "det")


def fetch(value, source_of):
    dets = lax.axis_size("det")
    pairs = []
    for place in range(lax.axis_size("tmpl")):
        for det in range(dets):
            source, source_det = source_of(place, det)
            pairs.append((source * dets + source_det, place * dets + det))
    return lax.ppermute(value, BOTH, pairs)


def from_ahead(value, steps):
    count = lax.axis_size("tmpl") * lax.axis_size("det")
    return lax.ppermute(value, BOTH, [((i + steps) % count, i) for i in range(count)])


def gather_part(part):
    places = lax.axis_size("tmpl")
    row = math.gcd(places, ROW)
    rows = places // row

    def along_x(steps, place, det):
        sign = 1 - 2 * det
        z, x = divmod(place, row)
        return z * row + (x + sign * steps) % row, det

    def along_z(steps, place, det):
        sign = 1 - 2 * det
        z, x = divmod(place, row)
        return (z + sign * steps) % rows * row + x, det

    held = part[None]
    steps = row // 2
    while steps:
        held = jnp.concatenate([held, fetch(held, functools.partial(along_x, steps))])
        steps //= 2
    across = held[None]
    steps = rows // 2
    while steps:
        across = jnp.concatenate([across, fetch(across, functools.partial(along_z, steps))])
        steps //= 2
    return across


def slot_of(steps, count):
    slot, bit = jnp.int32(0), 1
    while bit < count:
        slot = slot + lax.rem(lax.div(steps, bit), 2) * (count // 2 // bit)
        bit *= 2
    return slot


def peaks_kernel(place_ref, slid_ref, mine_ref, other_ref, out_ref, power_ref):
    x0, sign = place_ref[1], place_ref[2]
    row = mine_ref.shape[1]
    for detector in range(DETS):
        pieces = []
        for ref, way in ((mine_ref, sign), (other_ref, -sign)):
            for x in range(row):
                steps = lax.rem(way * (x - x0) + 2 * row, row)
                pieces.append(ref[0, slot_of(steps, row), detector])
        bank = jnp.concatenate(pieces, axis=0)
        filtered = lax.dot_general(
            slid_ref[detector], bank, (((1,), (1,)), ((), ())),
            preferred_element_type=jnp.float32,
        )
        squared = filtered * filtered
        half = squared.shape[1] // 2
        added = squared[:, :half] + squared[:, half:]
        if detector == 0:
            power_ref[...] = added
        elif detector < DETS - 1:
            power_ref[...] += added
        else:
            power = power_ref[...] + added
            windows = power.shape[0] // WIN
            peak = jnp.max(power.reshape(windows, WIN, half), axis=1)
            out_ref[...] = jnp.sqrt(peak)


def window_peaks(place, slid, mine, other):
    rows, row = mine.shape[:2]
    shard = mine.shape[3]
    block_len = slid.shape[1]
    tile = row * shard

    def slot(way, z, place_ref):
        steps = lax.rem(way * place_ref[2] * (z - place_ref[0]) + 2 * rows, rows)
        return slot_of(steps, rows)

    block = (1,) + mine.shape[1:]
    return pl.pallas_call(
        peaks_kernel,
        grid_spec=pltpu.PrefetchScalarGridSpec(
            num_scalar_prefetch=1,
            grid=(rows,),
            in_specs=[
                pl.BlockSpec(slid.shape, lambda z, p: (0, 0, 0)),
                pl.BlockSpec(block, lambda z, p: (slot(1, z, p), 0, 0, 0, 0)),
                pl.BlockSpec(block, lambda z, p: (slot(-1, z, p), 0, 0, 0, 0)),
            ],
            out_specs=pl.BlockSpec((block_len // WIN, tile), lambda z, p: (0, z)),
            scratch_shapes=[pltpu.VMEM((block_len, tile), jnp.float32)],
        ),
        out_shape=jax.ShapeDtypeStruct((block_len // WIN, rows * tile), jnp.float32),
        cost_estimate=pl.CostEstimate(
            flops=2 * 2 * DETS * rows * tile * block_len * slid.shape[2],
            bytes_accessed=2 * (slid.size + 2 * mine.size),
            transcendentals=0,
        ),
        name="peaks",
    )(place, slid, mine, other)


def per_device(basis_series, reconstruction, offsets):
    block_len = basis_series.shape[2]
    places = lax.axis_size("tmpl")
    row = math.gcd(places, ROW)
    place = lax.axis_index("tmpl")
    det = lax.axis_index("det")

    part = lax.dynamic_index_in_dim(reconstruction, det, 2, keepdims=False)
    mine = gather_part(part)
    other = fetch(mine, lambda at, core: (at, 1 - core))

    blocks_moved = lax.div(offsets, block_len)
    remainder = lax.rem(offsets, block_len)
    moved = []
    for detector in range(DETS):
        branches = [
            functools.partial(lambda value, steps: from_ahead(value, steps), steps=steps)
            for steps in range(SLIDES)
        ]
        moved.append(lax.switch(blocks_moved[detector], branches, basis_series[detector]))
    current = jnp.stack(moved)
    following = from_ahead(current, 1)
    joined = jnp.concatenate([current, following], axis=2)
    slid = jnp.stack(
        [
            lax.dynamic_slice_in_dim(joined[detector], remainder[detector], block_len, 1).T
            for detector in range(DETS)
        ]
    )

    where = jnp.stack([place // row, place % row, 1 - 2 * det]).astype(jnp.int32)
    return window_peaks(where, slid, mine, other).T


def solution(mesh):
    in_specs = (
        P(None, None, ("groups", "tmpl", "det")),
        P(None, ("groups", "tmpl"), None, None),
        P("groups"),
    )
    out_specs = P(None, ("groups", "tmpl", "det"))
    return jax.shard_map(
        per_device, mesh=mesh, in_specs=in_specs, out_specs=out_specs, check_vma=False
    )
```

```python
import functools
import math

import jax
import jax.numpy as jnp
from jax import lax
from jax.experimental import pallas as pl
from jax.experimental.pallas import tpu as pltpu
from jax.sharding import PartitionSpec as P

DETS = 3
WIN = 128
SLIDES = 16
ROW = 8
BOTH = ("tmpl", "det")


def fetch(value, source_of):
    dets = lax.axis_size("det")
    pairs = []
    for place in range(lax.axis_size("tmpl")):
        for det in range(dets):
            source, source_det = source_of(place, det)
            pairs.append((source * dets + source_det, place * dets + det))
    return lax.ppermute(value, BOTH, pairs)


def from_ahead(value, steps):
    count = lax.axis_size("tmpl") * lax.axis_size("det")
    return lax.ppermute(value, BOTH, [((i + steps) % count, i) for i in range(count)])


def after(value, *others):
    return lax.optimization_barrier((value, *others))[0]


def step_along(axis_is_x, steps):
    row = math.gcd(lax.axis_size("tmpl"), ROW)
    rows = lax.axis_size("tmpl") // row

    def source_of(place, det):
        shift = (1 - 2 * det) * steps
        z, x = divmod(place, row)
        if axis_is_x:
            return z * row + (x + shift) % row, det
        return (z + shift) % rows * row + x, det

    return functools.partial(fetch, source_of=source_of)


def slot_of(steps, count):
    slot, bit = jnp.int32(0), 1
    while bit < count:
        slot = slot + lax.rem(lax.div(steps, bit), 2) * (count // 2 // bit)
        bit *= 2
    return slot


def peaks_kernel(place_ref, slid_ref, mine_ref, other_ref, *refs):
    out_ref, power_ref = refs[-2:]
    x0, sign = place_ref[1], place_ref[2]
    row = mine_ref.shape[1]
    for detector in range(DETS):
        pieces = []
        for ref, way in ((mine_ref, sign), (other_ref, -sign)):
            for x in range(row):
                steps = lax.rem(way * (x - x0) + 2 * row, row)
                pieces.append(ref[0, slot_of(steps, row), detector])
        bank = jnp.concatenate(pieces, axis=0)
        filtered = lax.dot_general(
            slid_ref[detector], bank, (((1,), (1,)), ((), ())),
            preferred_element_type=jnp.float32,
        )
        squared = filtered * filtered
        half = squared.shape[1] // 2
        added = squared[:, :half] + squared[:, half:]
        if detector == 0:
            power_ref[...] = added
        elif detector < DETS - 1:
            power_ref[...] += added
        else:
            power = power_ref[...] + added
            windows = power.shape[0] // WIN
            peak = jnp.max(power.reshape(windows, WIN, half), axis=1)
            out_ref[...] = jnp.sqrt(peak)


def window_peaks(place, slid, mine, other, odd, so_far=None):
    halfrows, row = mine.shape[:2]
    rows = 2 * halfrows
    block_len = slid.shape[1]
    tile = row * mine.shape[3]

    def z_of(i, p):
        return lax.rem(p[0] + odd + 2 * i, rows)

    def held(way):
        def index(i, p):
            steps = lax.rem(way * p[2] * (z_of(i, p) - p[0]) + 2 * rows, rows)
            return slot_of(lax.div(steps, 2), halfrows), 0, 0, 0, 0

        return pl.BlockSpec((1,) + mine.shape[1:], index)

    in_specs = [pl.BlockSpec(slid.shape, lambda i, p: (0, 0, 0)), held(1), held(-1)]
    args = [place, slid, mine, other]
    if so_far is not None:
        in_specs.append(pl.BlockSpec(memory_space=pl.ANY))
        args.append(so_far)
    return pl.pallas_call(
        peaks_kernel,
        grid_spec=pltpu.PrefetchScalarGridSpec(
            num_scalar_prefetch=1,
            grid=(halfrows,),
            in_specs=in_specs,
            out_specs=pl.BlockSpec((block_len // WIN, tile), lambda i, p: (0, z_of(i, p))),
            scratch_shapes=[pltpu.VMEM((block_len, tile), jnp.float32)],
        ),
        out_shape=jax.ShapeDtypeStruct((block_len // WIN, rows * tile), jnp.float32),
        input_output_aliases={} if so_far is None else {4: 0},
        cost_estimate=pl.CostEstimate(
            flops=2 * 2 * DETS * halfrows * tile * block_len * slid.shape[2],
            bytes_accessed=2 * (slid.size + 2 * mine.size),
            transcendentals=0,
        ),
        name="peaks",
    )(*args)


def per_device(basis_series, reconstruction, offsets):
    block_len = basis_series.shape[2]
    places = lax.axis_size("tmpl")
    row = math.gcd(places, ROW)
    rows = places // row
    place = lax.axis_index("tmpl")
    det = lax.axis_index("det")
    where = jnp.stack([place // row, place % row, 1 - 2 * det]).astype(jnp.int32)
    blocks_moved = lax.div(offsets, block_len)
    remainder = lax.rem(offsets, block_len)

    branches = [functools.partial(from_ahead, steps=steps) for steps in range(SLIDES)]

    def slide(detector, *others):
        series = after(basis_series[detector], *others) if others else basis_series[detector]
        return lax.switch(blocks_moved[detector], branches, series)

    def swap(value):
        return fetch(value, lambda at, core: (at, 1 - core))

    held = lax.dynamic_index_in_dim(reconstruction, det, 2, keepdims=False)[None]
    moved = []
    steps = row // 2
    while steps:
        got = step_along(True, steps)(held)
        if not moved:
            moved.append(slide(0))
            got = after(got, moved[0])
        held = jnp.concatenate([held, got])
        steps //= 2
    across = held[None]
    steps = rows // 2
    following = None
    while steps > 1:
        got = step_along(False, steps)(across)
        if len(moved) < DETS:
            moved.append(slide(len(moved), across))
            got = after(got, moved[-1])
        elif following is None:
            current = jnp.stack(moved)
            following = from_ahead(after(current, across), 1)
            got = after(got, following)
        across = jnp.concatenate([across, got])
        steps //= 2

    far = step_along(False, 1)(across)
    near_other = swap(across)
    joined = jnp.concatenate([current, following], axis=2)
    slid = jnp.stack(
        [
            lax.dynamic_slice_in_dim(joined[detector], remainder[detector], block_len, 1).T
            for detector in range(DETS)
        ]
    )
    peaks = window_peaks(where, slid, across, near_other, 0)
    far = after(far, peaks)
    return window_peaks(where, slid, far, swap(far), 1, peaks).T


def solution(mesh):
    in_specs = (
        P(None, None, ("groups", "tmpl", "det")),
        P(None, ("groups", "tmpl"), None, None),
        P("groups"),
    )
    out_specs = P(None, ("groups", "tmpl", "det"))
    return jax.shard_map(
        per_device, mesh=mesh, in_specs=in_specs, out_specs=out_specs, check_vma=False
    )
```

```python
import functools
import math

import jax
import jax.numpy as jnp
from jax import lax
from jax.experimental import pallas as pl
from jax.experimental.pallas import tpu as pltpu
from jax.sharding import PartitionSpec as P

DETS = 3
WIN = 128
SLIDES = 16
ROW = 8
FAN = 4
BOTH = ("tmpl", "det")


def fetch(value, source_of):
    dets = lax.axis_size("det")
    pairs = []
    for place in range(lax.axis_size("tmpl")):
        for det in range(dets):
            source, source_det = source_of(place, det)
            pairs.append((source * dets + source_det, place * dets + det))
    return lax.ppermute(value, BOTH, pairs)


def from_ahead(value, steps):
    count = lax.axis_size("tmpl") * lax.axis_size("det")
    return lax.ppermute(value, BOTH, [((i + steps) % count, i) for i in range(count)])


def after(value, *others):
    return lax.optimization_barrier((value, *others))[0]


def step_along(axis_is_x, steps):
    row = math.gcd(lax.axis_size("tmpl"), ROW)
    rows = lax.axis_size("tmpl") // row

    def source_of(place, det):
        shift = (1 - 2 * det) * steps
        z, x = divmod(place, row)
        if axis_is_x:
            return z * row + (x + shift) % row, det
        return (z + shift) % rows * row + x, det

    return functools.partial(fetch, source_of=source_of)


def slot_of(steps, rows):
    short = lax.rem(steps, FAN)
    quads = lax.rem(lax.div(steps + lax.div(short, FAN - 1), FAN), rows // FAN)
    return short * (rows // FAN) + quads


def peaks_kernel(place_ref, slid_ref, mine_ref, other_ref, out_ref, power_ref):
    z0, x0, sign = place_ref[0], place_ref[1], place_ref[2]
    rows, row = mine_ref.shape[:2]
    half = row * mine_ref.shape[3]

    def tile(z, _):
        sides = []
        for ref, way in ((mine_ref, sign), (other_ref, -sign)):
            sides.append((ref, way, slot_of(lax.rem(way * (z - z0) + 2 * rows, rows), rows)))
        for detector in range(DETS):
            pieces = []
            for ref, way, slot in sides:
                for x in range(row):
                    pieces.append(ref[slot, lax.rem(way * (x - x0) + 2 * row, row), detector])
            bank = jnp.concatenate(pieces, axis=0)
            filtered = lax.dot_general(
                slid_ref[detector], bank, (((1,), (1,)), ((), ())),
                preferred_element_type=jnp.float32,
            )
            squared = filtered * filtered
            added = squared[:, :half] + squared[:, half:]
            if detector == 0:
                power_ref[...] = added
            elif detector < DETS - 1:
                power_ref[...] += added
            else:
                power = power_ref[...] + added
                windows = power.shape[0] // WIN
                peak = jnp.max(power.reshape(windows, WIN, half), axis=1)
                out_ref[:, pl.ds(pl.multiple_of(z * half, half), half)] = jnp.sqrt(peak)
        return 0

    lax.fori_loop(0, rows, tile, 0)


def window_peaks(place, slid, mine, other):
    rows, row = mine.shape[:2]
    block_len = slid.shape[1]
    tile = row * mine.shape[3]
    whole = pl.BlockSpec(memory_space=pltpu.VMEM)
    return pl.pallas_call(
        peaks_kernel,
        in_specs=[pl.BlockSpec(memory_space=pltpu.SMEM), whole, whole, whole],
        out_specs=whole,
        scratch_shapes=[pltpu.VMEM((block_len, tile), jnp.float32)],
        out_shape=jax.ShapeDtypeStruct((block_len // WIN, rows * tile), jnp.float32),
        cost_estimate=pl.CostEstimate(
            flops=2 * 2 * DETS * rows * tile * block_len * slid.shape[2],
            bytes_accessed=2 * (slid.size + 2 * mine.size),
            transcendentals=0,
        ),
        name="peaks",
    )(place, slid, mine, other)


def per_device(basis_series, reconstruction, offsets):
    block_len = basis_series.shape[2]
    places = lax.axis_size("tmpl")
    row = math.gcd(places, ROW)
    rows = places // row
    place = lax.axis_index("tmpl")
    det = lax.axis_index("det")
    where = jnp.stack([place // row, place % row, 1 - 2 * det]).astype(jnp.int32)
    blocks_moved = lax.div(offsets, block_len)
    remainder = lax.rem(offsets, block_len)

    branches = [functools.partial(from_ahead, steps=steps) for steps in range(SLIDES)]

    def slide(detector, *others):
        series = after(basis_series[detector], *others) if others else basis_series[detector]
        return lax.switch(blocks_moved[detector], branches, series)

    part = lax.dynamic_index_in_dim(reconstruction, det, 2, keepdims=False)
    got = [step_along(True, steps)(part) for steps in range(1, row)]
    moved = [slide(0)]
    held = jnp.stack([part] + [after(piece, moved[0]) for piece in got])

    got = [step_along(False, steps)(held) for steps in range(FAN, rows, FAN)]
    moved.append(slide(1, held))
    quads = jnp.stack([held] + [after(piece, moved[1]) for piece in got])

    got = [step_along(False, steps)(quads) for steps in (1, 2, -1)]
    moved.append(slide(2, quads))
    current = jnp.stack(moved)
    following = from_ahead(current, 1)
    mine = jnp.concatenate([quads] + [after(piece, moved[2]) for piece in got])
    other = fetch(mine, lambda at, core: (at, 1 - core))

    joined = jnp.concatenate([current, following], axis=2)
    slid = jnp.stack(
        [
            lax.dynamic_slice_in_dim(joined[detector], remainder[detector], block_len, 1).T
            for detector in range(DETS)
        ]
    )
    return window_peaks(where, slid, mine, other).T


def solution(mesh):
    in_specs = (
        P(None, None, ("groups", "tmpl", "det")),
        P(None, ("groups", "tmpl"), None, None),
        P("groups"),
    )
    out_specs = P(None, ("groups", "tmpl", "det"))
    return jax.shard_map(
        per_device, mesh=mesh, in_specs=in_specs, out_specs=out_specs, check_vma=False
    )
```

```python
import functools
import math

import jax
import jax.numpy as jnp
from jax import lax
from jax.experimental import pallas as pl
from jax.experimental.pallas import tpu as pltpu
from jax.sharding import PartitionSpec as P

DETS = 3
WIN = 128
SLIDES = 16
ROW = 8
FAN = 4
BOTH = ("tmpl", "det")


def fetch(value, source_of):
    dets = lax.axis_size("det")
    pairs = []
    for place in range(lax.axis_size("tmpl")):
        for det in range(dets):
            source, source_det = source_of(place, det)
            pairs.append((source * dets + source_det, place * dets + det))
    return lax.ppermute(value, BOTH, pairs)


def from_ahead(value, steps):
    if steps == 0:
        return value
    count = lax.axis_size("tmpl") * lax.axis_size("det")
    return lax.ppermute(value, BOTH, [((i + steps) % count, i) for i in range(count)])


def after(value, *others):
    return lax.optimization_barrier((value, *others))[0]


def step_along(axis_is_x, steps):
    row = math.gcd(lax.axis_size("tmpl"), ROW)
    rows = lax.axis_size("tmpl") // row

    def source_of(place, det):
        shift = (1 - 2 * det) * steps
        z, x = divmod(place, row)
        if axis_is_x:
            return z * row + (x + shift) % row, det
        return (z + shift) % rows * row + x, det

    return functools.partial(fetch, source_of=source_of)


def x_slot_of(steps, row):
    slot, bit = jnp.int32(0), 1
    while bit < row:
        slot = slot + lax.rem(lax.div(steps, bit), 2) * (row // 2 // bit)
        bit *= 2
    return slot


def slot_of(steps, rows):
    short = lax.rem(steps, FAN)
    quads = lax.rem(lax.div(steps + lax.div(short, FAN - 1), FAN), rows // FAN)
    return short * (rows // FAN) + quads


def peaks_kernel(place_ref, order_ref, slid_ref, mine_ref, other_ref, out_ref, power_ref):
    z0, x0, sign = place_ref[0], place_ref[1], place_ref[2]
    rows, row = mine_ref.shape[:2]
    half = row * mine_ref.shape[3]

    def tile(z, _):
        sides = []
        for ref, way in ((mine_ref, sign), (other_ref, -sign)):
            sides.append((ref, way, slot_of(lax.rem(way * (z - z0) + 2 * rows, rows), rows)))
        for detector in range(DETS):
            pieces = []
            for ref, way, slot in sides:
                for x in range(row):
                    steps = lax.rem(way * (x - x0) + 2 * row, row)
                    pieces.append(ref[slot, x_slot_of(steps, row), order_ref[detector]])
            bank = jnp.concatenate(pieces, axis=0)
            filtered = lax.dot_general(
                slid_ref[detector], bank, (((1,), (1,)), ((), ())),
                preferred_element_type=jnp.float32,
            )
            squared = filtered * filtered
            added = squared[:, :half] + squared[:, half:]
            if detector == 0:
                power_ref[...] = added
            elif detector < DETS - 1:
                power_ref[...] += added
            else:
                power = power_ref[...] + added
                windows = power.shape[0] // WIN
                peak = jnp.max(power.reshape(windows, WIN, half), axis=1)
                out_ref[:, pl.ds(pl.multiple_of(z * half, half), half)] = jnp.sqrt(peak)
        return 0

    lax.fori_loop(0, rows, tile, 0)


def window_peaks(place, order, slid, mine, other):
    rows, row = mine.shape[:2]
    block_len = slid.shape[1]
    tile = row * mine.shape[3]
    whole = pl.BlockSpec(memory_space=pltpu.VMEM)
    return pl.pallas_call(
        peaks_kernel,
        in_specs=[pl.BlockSpec(memory_space=pltpu.SMEM)] * 2 + [whole] * 3,
        out_specs=whole,
        scratch_shapes=[pltpu.VMEM((block_len, tile), jnp.float32)],
        out_shape=jax.ShapeDtypeStruct((block_len // WIN, rows * tile), jnp.float32),
        cost_estimate=pl.CostEstimate(
            flops=2 * 2 * DETS * rows * tile * block_len * slid.shape[2],
            bytes_accessed=2 * (slid.size + 2 * mine.size),
            transcendentals=0,
        ),
        name="peaks",
    )(place, order, slid, mine, other)


def per_device(basis_series, reconstruction, offsets):
    block_len = basis_series.shape[2]
    places = lax.axis_size("tmpl")
    row = math.gcd(places, ROW)
    rows = places // row
    place = lax.axis_index("tmpl")
    det = lax.axis_index("det")
    where = jnp.stack([place // row, place % row, 1 - 2 * det]).astype(jnp.int32)
    blocks_moved = lax.div(offsets, block_len)

    places_of = jnp.arange(DETS)
    before = (blocks_moved[None] < blocks_moved[:, None]) | (
        (blocks_moved[None] == blocks_moved[:, None]) & (places_of[None] < places_of[:, None])
    )
    rank = jnp.sum(before.astype(jnp.int32), axis=1)
    order = jnp.sum(jnp.where(rank[None] == places_of[:, None], places_of[None], 0), axis=1)
    order = order.astype(jnp.int32)
    low, middle, high = (blocks_moved[order[i]] for i in range(DETS))
    down, up = middle - low, high - middle
    branches = []
    for back in range(SLIDES):
        for ahead in range(SLIDES - back):
            branches.append(
                lambda one, two, back=back, ahead=ahead: (
                    from_ahead(one, -back),
                    from_ahead(two, ahead),
                )
            )
    branch = down * SLIDES - lax.div(down * (down - 1), 2) + up

    held = lax.dynamic_index_in_dim(reconstruction, det, 2, keepdims=False)[None]
    steps = row // 2
    while steps:
        held = jnp.concatenate([held, step_along(True, steps)(held)])
        steps //= 2

    got = [step_along(False, steps)(held) for steps in range(FAN, rows, FAN)]
    series = after(basis_series, held)
    one, still, two = (
        lax.dynamic_index_in_dim(series, order[i], 0, keepdims=False) for i in range(DETS)
    )
    one, two = lax.switch(branch, branches, one, two)
    quads = jnp.stack([held] + [after(piece, one, two) for piece in got])

    got = [step_along(False, steps)(quads) for steps in (1, 2, -1)]
    current = jnp.stack([one, still, two])
    following = from_ahead(after(current, quads), 1)
    mine = jnp.concatenate([quads] + [after(piece, following) for piece in got])
    other = fetch(mine, lambda at, core: (at, 1 - core))

    joined = jnp.concatenate([current, following], axis=2)
    remainder = lax.rem(offsets, block_len)
    slid = jnp.stack(
        [
            lax.dynamic_slice_in_dim(joined[i], remainder[order[i]], block_len, 1).T
            for i in range(DETS)
        ]
    )
    peaks = window_peaks(where, order, slid, mine, other)
    home = [functools.partial(from_ahead, steps=steps) for steps in range(SLIDES)]
    return lax.switch(middle, home, peaks).T


def solution(mesh):
    in_specs = (
        P(None, None, ("groups", "tmpl", "det")),
        P(None, ("groups", "tmpl"), None, None),
        P("groups"),
    )
    out_specs = P(None, ("groups", "tmpl", "det"))
    return jax.shard_map(
        per_device, mesh=mesh, in_specs=in_specs, out_specs=out_specs, check_vma=False
    )
```

```python
import functools
import math

import jax
import jax.numpy as jnp
from jax import lax
from jax.experimental import pallas as pl
from jax.experimental.pallas import tpu as pltpu
from jax.sharding import PartitionSpec as P

DETS = 3
WIN = 128
SLIDES = 16
ROW = 8
FAN = 4
BOTH = ("tmpl", "det")


def fetch(value, source_of):
    dets = lax.axis_size("det")
    pairs = []
    for place in range(lax.axis_size("tmpl")):
        for det in range(dets):
            source, source_det = source_of(place, det)
            pairs.append((source * dets + source_det, place * dets + det))
    return lax.ppermute(value, BOTH, pairs)


def from_ahead(value, steps):
    if steps == 0:
        return value
    count = lax.axis_size("tmpl") * lax.axis_size("det")
    return lax.ppermute(value, BOTH, [((i + steps) % count, i) for i in range(count)])


def after(value, *others):
    return lax.optimization_barrier((value, *others))[0]


def step_along(axis_is_x, steps):
    row = math.gcd(lax.axis_size("tmpl"), ROW)
    rows = lax.axis_size("tmpl") // row

    def source_of(place, det):
        shift = (1 - 2 * det) * steps
        z, x = divmod(place, row)
        if axis_is_x:
            return z * row + (x + shift) % row, det
        return (z + shift) % rows * row + x, det

    return functools.partial(fetch, source_of=source_of)


def x_slot_of(steps, row):
    slot, bit = jnp.int32(0), 1
    while bit < row:
        slot = slot + lax.rem(lax.div(steps, bit), 2) * (row // 2 // bit)
        bit *= 2
    return slot


def slot_of(steps, rows):
    short = lax.rem(steps, FAN)
    quads = lax.rem(lax.div(steps + lax.div(short, FAN - 1), FAN), rows // FAN)
    return short * (rows // FAN) + quads


def peaks_kernel(place_ref, order_ref, slid_ref, mine_ref, other_ref, out_ref, power_ref):
    z0, x0, sign = place_ref[0], place_ref[1], place_ref[2]
    rows, row = mine_ref.shape[:2]
    half = row * mine_ref.shape[3]

    def tile(z, _):
        sides = []
        for ref, way in ((mine_ref, sign), (other_ref, -sign)):
            sides.append((ref, way, slot_of(lax.rem(way * (z - z0) + 2 * rows, rows), rows)))
        for detector in range(DETS):
            pieces = []
            for ref, way, slot in sides:
                for x in range(row):
                    steps = lax.rem(way * (x - x0) + 2 * row, row)
                    pieces.append(ref[slot, x_slot_of(steps, row), order_ref[detector]])
            bank = jnp.concatenate(pieces, axis=0)
            filtered = lax.dot_general(
                slid_ref[detector], bank, (((1,), (1,)), ((), ())),
                preferred_element_type=jnp.float32,
            )
            squared = filtered * filtered
            added = squared[:, :half] + squared[:, half:]
            if detector == 0:
                power_ref[...] = added
            elif detector < DETS - 1:
                power_ref[...] += added
            else:
                power = power_ref[...] + added
                windows = power.shape[0] // WIN
                peak = jnp.max(power.reshape(windows, WIN, half), axis=1)
                out_ref[:, pl.ds(pl.multiple_of(z * half, half), half)] = jnp.sqrt(peak)
        return 0

    lax.fori_loop(0, rows, tile, 0)


def window_peaks(place, order, slid, mine, other):
    rows, row = mine.shape[:2]
    block_len = slid.shape[1]
    tile = row * mine.shape[3]
    whole = pl.BlockSpec(memory_space=pltpu.VMEM)
    return pl.pallas_call(
        peaks_kernel,
        in_specs=[pl.BlockSpec(memory_space=pltpu.SMEM)] * 2 + [whole] * 3,
        out_specs=whole,
        scratch_shapes=[pltpu.VMEM((block_len, tile), jnp.float32)],
        out_shape=jax.ShapeDtypeStruct((block_len // WIN, rows * tile), jnp.float32),
        cost_estimate=pl.CostEstimate(
            flops=2 * 2 * DETS * rows * tile * block_len * slid.shape[2],
            bytes_accessed=2 * (slid.size + 2 * mine.size),
            transcendentals=0,
        ),
        name="peaks",
    )(place, order, slid, mine, other)


def per_device(basis_series, reconstruction, offsets):
    block_len = basis_series.shape[2]
    places = lax.axis_size("tmpl")
    row = math.gcd(places, ROW)
    rows = places // row
    place = lax.axis_index("tmpl")
    det = lax.axis_index("det")
    where = jnp.stack([place // row, place % row, 1 - 2 * det]).astype(jnp.int32)
    blocks_moved = lax.div(offsets, block_len)

    places_of = jnp.arange(DETS)
    before = (blocks_moved[None] < blocks_moved[:, None]) | (
        (blocks_moved[None] == blocks_moved[:, None]) & (places_of[None] < places_of[:, None])
    )
    rank = jnp.sum(before.astype(jnp.int32), axis=1)
    order = jnp.sum(jnp.where(rank[None] == places_of[:, None], places_of[None], 0), axis=1)
    order = order.astype(jnp.int32)
    low, middle, high = (blocks_moved[order[i]] for i in range(DETS))
    down, up = middle - low, high - middle
    backward = [functools.partial(from_ahead, steps=-steps) for steps in range(SLIDES)]
    forward = [functools.partial(from_ahead, steps=steps) for steps in range(SLIDES)]

    held = lax.dynamic_index_in_dim(reconstruction, det, 2, keepdims=False)[None]
    steps = row // 2
    while steps:
        held = jnp.concatenate([held, step_along(True, steps)(held)])
        steps //= 2

    got = [step_along(False, steps)(held) for steps in range(FAN, rows, FAN)]
    series = after(basis_series, held)
    one, still, two = (
        lax.dynamic_index_in_dim(series, order[i], 0, keepdims=False) for i in range(DETS)
    )
    one = lax.switch(down, backward, one)
    quads = jnp.stack([held] + [after(piece, one) for piece in got])

    got = [step_along(False, steps)(quads) for steps in (1, 2, -1)]
    two = lax.switch(up, forward, after(two, quads))
    current = jnp.stack([one, still, two])
    following = from_ahead(current, 1)
    mine = jnp.concatenate([quads] + [after(piece, two) for piece in got])
    other = fetch(mine, lambda at, core: (at, 1 - core))

    joined = jnp.concatenate([current, following], axis=2)
    remainder = lax.rem(offsets, block_len)
    slid = jnp.stack(
        [
            lax.dynamic_slice_in_dim(joined[i], remainder[order[i]], block_len, 1).T
            for i in range(DETS)
        ]
    )
    peaks = window_peaks(where, order, slid, mine, other)
    return lax.switch(middle, forward, peaks).T


def solution(mesh):
    in_specs = (
        P(None, None, ("groups", "tmpl", "det")),
        P(None, ("groups", "tmpl"), None, None),
        P("groups"),
    )
    out_specs = P(None, ("groups", "tmpl", "det"))
    return jax.shard_map(
        per_device, mesh=mesh, in_specs=in_specs, out_specs=out_specs, check_vma=False
    )
```

```python
import functools
import math

import jax
import jax.numpy as jnp
from jax import lax
from jax.experimental import pallas as pl
from jax.experimental.pallas import tpu as pltpu
from jax.sharding import PartitionSpec as P

DETS = 3
WIN = 128
SLIDES = 16
ROW = 8
FAN = 4
ROW_TILE = 128
BOTH = ("tmpl", "det")


def fetch(value, source_of):
    dets = lax.axis_size("det")
    pairs = []
    for place in range(lax.axis_size("tmpl")):
        for det in range(dets):
            source, source_det = source_of(place, det)
            pairs.append((source * dets + source_det, place * dets + det))
    return lax.ppermute(value, BOTH, pairs)


def from_ahead(value, steps):
    if steps == 0:
        return value
    count = lax.axis_size("tmpl") * lax.axis_size("det")
    return lax.ppermute(value, BOTH, [((i + steps) % count, i) for i in range(count)])


def after(value, *others):
    return lax.optimization_barrier((value, *others))[0]


def fetch_z(value, steps):
    places = lax.axis_size("tmpl")
    row = math.gcd(places, ROW)
    return fetch(value, lambda at, det: ((at + (1 - 2 * det) * steps * row) % places, det))


def x_slot_of(steps, row):
    slot, bit = jnp.zeros_like(steps), 1
    while bit < row:
        slot = slot + lax.rem(lax.div(steps, bit), 2) * (row // 2 // bit)
        bit *= 2
    return slot


def slot_of(steps, rows):
    short = lax.rem(steps, FAN)
    quads = lax.rem(lax.div(steps + lax.div(short, FAN - 1), FAN), rows // FAN)
    return short * (rows // FAN) + quads


def peaks_kernel(table_ref, order_ref, slid_ref, mine_ref, other_ref, out_ref, power_ref):
    row = ROW_TILE // mine_ref.shape[2]
    half = row * mine_ref.shape[2]

    def tile(z, _):
        for detector in range(DETS):
            pieces = []
            for side, ref in enumerate((mine_ref, other_ref)):
                for x in range(row):
                    pieces.append(ref[table_ref[side, z * row + x], order_ref[detector]])
            bank = jnp.concatenate(pieces, axis=0)
            filtered = lax.dot_general(
                slid_ref[detector], bank, (((1,), (1,)), ((), ())),
                preferred_element_type=jnp.float32,
            )
            squared = filtered * filtered
            added = squared[:, :half] + squared[:, half:]
            if detector == 0:
                power_ref[...] = added
            elif detector < DETS - 1:
                power_ref[...] += added
            else:
                power = power_ref[...] + added
                windows = power.shape[0] // WIN
                peak = jnp.max(power.reshape(windows, WIN, half), axis=1)
                out_ref[:, pl.ds(pl.multiple_of(z * half, half), half)] = jnp.sqrt(peak)
        return 0

    lax.fori_loop(0, out_ref.shape[1] // half, tile, 0)


def window_peaks(table, order, slid, mine, other):
    block_len = slid.shape[1]
    templates = mine.shape[0] * mine.shape[2]
    whole = pl.BlockSpec(memory_space=pltpu.VMEM)
    return pl.pallas_call(
        peaks_kernel,
        in_specs=[pl.BlockSpec(memory_space=pltpu.SMEM)] * 2 + [whole] * 3,
        out_specs=whole,
        scratch_shapes=[pltpu.VMEM((block_len, ROW_TILE), jnp.float32)],
        out_shape=jax.ShapeDtypeStruct((block_len // WIN, templates), jnp.float32),
        cost_estimate=pl.CostEstimate(
            flops=2 * 2 * DETS * templates * block_len * slid.shape[2],
            bytes_accessed=2 * (slid.size + 2 * mine.size),
            transcendentals=0,
        ),
        name="peaks",
    )(table, order, slid, mine, other)


def per_device(basis_series, reconstruction, offsets):
    block_len = basis_series.shape[2]
    places = lax.axis_size("tmpl")
    dets = lax.axis_size("det")
    row = math.gcd(places, ROW)
    rows = places // row
    det = lax.axis_index("det")

    away = lax.rem(jnp.arange(places) - lax.axis_index("tmpl") + places, places)
    x_slot = x_slot_of(lax.rem(away, row), row)
    z_away = lax.div(away, row)
    looked_up = slot_of(z_away, rows) * row + x_slot
    looked_down = slot_of(lax.rem(rows - z_away, rows), rows) * row + x_slot
    table = jnp.stack(
        [
            jnp.where(det == 0, looked_up, looked_down),
            jnp.where(det == 0, looked_down, looked_up),
        ]
    ).astype(jnp.int32)

    blocks_moved = lax.div(offsets, block_len)

    places_of = jnp.arange(DETS)
    before = (blocks_moved[None] < blocks_moved[:, None]) | (
        (blocks_moved[None] == blocks_moved[:, None]) & (places_of[None] < places_of[:, None])
    )
    rank = jnp.sum(before.astype(jnp.int32), axis=1)
    order = jnp.sum(jnp.where(rank[None] == places_of[:, None], places_of[None], 0), axis=1)
    order = order.astype(jnp.int32)
    low, middle, high = (blocks_moved[order[i]] for i in range(DETS))
    down, up = middle - low, high - middle
    backward = [functools.partial(from_ahead, steps=-steps) for steps in range(SLIDES - 1)]
    forward = [functools.partial(from_ahead, steps=steps) for steps in range(SLIDES - 1)]
    home = [functools.partial(from_ahead, steps=steps) for steps in range(1, SLIDES)]

    held = lax.dynamic_index_in_dim(reconstruction, det, 2, keepdims=False)[None]
    steps = row // 2
    while steps:
        held = jnp.concatenate([held, from_ahead(held, steps * dets)])
        steps //= 2

    got = [fetch_z(held, steps) for steps in range(FAN, rows, FAN)]
    series = after(basis_series, held)
    one, still, two = (
        lax.dynamic_index_in_dim(series, order[i], 0, keepdims=False) for i in range(DETS)
    )
    one = lax.switch(down, backward, one)
    quads = jnp.stack([held] + [after(piece, one) for piece in got])

    got = [fetch_z(quads, steps) for steps in (1, 2, -1)]
    two = lax.switch(up, forward, after(two, quads))
    current = jnp.stack([one, still, two])
    following = from_ahead(current, 1)
    mine = jnp.concatenate([quads] + [after(piece, two) for piece in got])
    other = fetch(mine, lambda at, core: (at, 1 - core))

    joined = jnp.concatenate([current, following], axis=2)
    remainder = lax.rem(offsets, block_len)
    slid = jnp.stack(
        [
            lax.dynamic_slice_in_dim(joined[i], remainder[order[i]], block_len, 1).T
            for i in range(DETS)
        ]
    )
    shape = (places,) + mine.shape[2:]
    peaks = window_peaks(table, order, slid, mine.reshape(shape), other.reshape(shape))
    return lax.switch(middle - 1, home, peaks).T


def solution(mesh):
    in_specs = (
        P(None, None, ("groups", "tmpl", "det")),
        P(None, ("groups", "tmpl"), None, None),
        P("groups"),
    )
    out_specs = P(None, ("groups", "tmpl", "det"))
    return jax.shard_map(
        per_device, mesh=mesh, in_specs=in_specs, out_specs=out_specs, check_vma=False
    )
```

```python
import functools
import math

import jax
import jax.numpy as jnp
from jax import lax
from jax.experimental import pallas as pl
from jax.experimental.pallas import tpu as pltpu
from jax.sharding import PartitionSpec as P

DETS = 3
WIN = 128
SLIDES = 16
ROW = 8
FAN = 4
ROW_TILE = 128
BOTH = ("tmpl", "det")


def fetch(value, source_of):
    dets = lax.axis_size("det")
    pairs = []
    for place in range(lax.axis_size("tmpl")):
        for det in range(dets):
            source, source_det = source_of(place, det)
            pairs.append((source * dets + source_det, place * dets + det))
    return lax.ppermute(value, BOTH, pairs)


def from_ahead(value, steps):
    if steps == 0:
        return value
    count = lax.axis_size("tmpl") * lax.axis_size("det")
    return lax.ppermute(value, BOTH, [((i + steps) % count, i) for i in range(count)])


def after(value, *others):
    return lax.optimization_barrier((value, *others))[0]


def fetch_z(value, steps):
    places = lax.axis_size("tmpl")
    row = math.gcd(places, ROW)
    return fetch(value, lambda at, det: ((at + (1 - 2 * det) * steps * row) % places, det))


def plan_kernel(block_len, offsets_ref, plan_ref):
    moved = [lax.div(offsets_ref[i], block_len) for i in range(DETS)]
    ranks = []
    for i in range(DETS):
        rank = jnp.int32(0)
        for j in range(DETS):
            if i != j:
                less = moved[j] <= moved[i] if j < i else moved[j] < moved[i]
                rank = rank + jnp.where(less, 1, 0)
        ranks.append(rank)
    by_rank = []
    for place in range(DETS):
        index, blocks, rest = jnp.int32(0), moved[0], offsets_ref[0]
        for i in range(1, DETS):
            index = jnp.where(ranks[i] == place, i, index)
            blocks = jnp.where(ranks[i] == place, moved[i], blocks)
            rest = jnp.where(ranks[i] == place, offsets_ref[i], rest)
        plan_ref[place] = index
        plan_ref[DETS + place] = lax.rem(rest, block_len)
        by_rank.append(blocks)
    plan_ref[2 * DETS] = by_rank[1] - by_rank[0]
    plan_ref[2 * DETS + 1] = by_rank[2] - by_rank[1]
    plan_ref[2 * DETS + 2] = by_rank[1] - 1


def plan_of(offsets, block_len):
    return pl.pallas_call(
        functools.partial(plan_kernel, block_len),
        in_specs=[pl.BlockSpec(memory_space=pltpu.SMEM)],
        out_specs=pl.BlockSpec(memory_space=pltpu.SMEM),
        out_shape=jax.ShapeDtypeStruct((3 * DETS,), jnp.int32),
        name="plan",
    )(offsets)


def reversed_bits(steps, count):
    slot, bit = jnp.int32(0), 1
    while bit < count:
        slot = slot + lax.rem(lax.div(steps, bit), 2) * (count // 2 // bit)
        bit *= 2
    return slot


def slot_of(steps, rows):
    short = lax.rem(steps, FAN)
    quads = lax.rem(lax.div(steps + lax.div(short, FAN - 1), FAN), rows // FAN)
    return short * (rows // FAN) + quads


def peaks_kernel(plan_ref, slid_ref, mine_ref, other_ref, out_ref, power_ref):
    row = ROW_TILE // mine_ref.shape[2]
    rows = mine_ref.shape[0] // row
    half = row * mine_ref.shape[2]
    place, down = lax.axis_index("tmpl"), lax.axis_index("det")
    z0, x0 = lax.div(place, row), lax.rem(place, row)
    x_slots = [reversed_bits(lax.rem(x - x0 + row, row), row) for x in range(row)]

    def tile(z, _):
        slots = []
        for behind in range(2):
            away = lax.rem(z - z0 - behind + 2 * rows, rows)
            looked_up = slot_of(away, rows) * row
            looked_down = slot_of(lax.rem(rows - away, rows), rows) * row
            slots.append(
                (
                    jnp.where(down == 0, looked_up, looked_down),
                    jnp.where(down == 0, looked_down, looked_up),
                )
            )
        for detector in range(DETS):
            pieces = []
            for side, ref in enumerate((mine_ref, other_ref)):
                for x in range(row):
                    slot = jnp.where(x < x0, slots[1][side], slots[0][side]) + x_slots[x]
                    pieces.append(ref[slot, plan_ref[detector]])
            bank = jnp.concatenate(pieces, axis=0)
            filtered = lax.dot_general(
                slid_ref[detector], bank, (((1,), (1,)), ((), ())),
                preferred_element_type=jnp.float32,
            )
            squared = filtered * filtered
            added = squared[:, :half] + squared[:, half:]
            if detector == 0:
                power_ref[...] = added
            elif detector < DETS - 1:
                power_ref[...] += added
            else:
                power = power_ref[...] + added
                windows = power.shape[0] // WIN
                peak = jnp.max(power.reshape(windows, WIN, half), axis=1)
                out_ref[:, pl.ds(pl.multiple_of(z * half, half), half)] = jnp.sqrt(peak)
        return 0

    lax.fori_loop(0, rows, tile, 0, unroll=2)


def window_peaks(plan, slid, mine, other):
    block_len = slid.shape[1]
    templates = mine.shape[0] * mine.shape[2]
    whole = pl.BlockSpec(memory_space=pltpu.VMEM)
    return pl.pallas_call(
        peaks_kernel,
        in_specs=[pl.BlockSpec(memory_space=pltpu.SMEM)] + [whole] * 3,
        out_specs=whole,
        scratch_shapes=[pltpu.VMEM((block_len, ROW_TILE), jnp.float32)],
        out_shape=jax.ShapeDtypeStruct((block_len // WIN, templates), jnp.float32),
        cost_estimate=pl.CostEstimate(
            flops=2 * 2 * DETS * templates * block_len * slid.shape[2],
            bytes_accessed=2 * (slid.size + 2 * mine.size),
            transcendentals=0,
        ),
        name="peaks",
    )(plan, slid, mine, other)


def per_device(basis_series, reconstruction, offsets):
    block_len = basis_series.shape[2]
    places = lax.axis_size("tmpl")
    dets = lax.axis_size("det")
    row = math.gcd(places, ROW)
    rows = places // row
    det = lax.axis_index("det")

    plan = plan_of(offsets, block_len)
    order = plan[:DETS].astype(jnp.uint32)
    remainder = plan[DETS : 2 * DETS].astype(jnp.uint32)
    down, up, middle = (plan[2 * DETS + i] for i in range(3))

    backward = [functools.partial(from_ahead, steps=-steps) for steps in range(SLIDES - 1)]
    forward = [functools.partial(from_ahead, steps=steps) for steps in range(SLIDES - 1)]
    home = [
        lambda value, steps=steps: from_ahead(value, steps).T for steps in range(1, SLIDES)
    ]

    held = lax.dynamic_index_in_dim(reconstruction, det, 2, keepdims=False)[None]
    steps = row // 2
    while steps:
        held = jnp.concatenate([held, from_ahead(held, steps * dets)])
        steps //= 2

    got = [fetch_z(held, steps) for steps in range(FAN, rows, FAN)]
    zero = jnp.uint32(0)
    one, still, two = (
        lax.dynamic_slice(basis_series, (order[i], zero, zero), (1,) + basis_series.shape[1:])[0]
        for i in range(DETS)
    )
    one = lax.switch(down, backward, after(one, held))
    quads = jnp.stack([held] + [after(piece, one) for piece in got])

    got = [fetch_z(quads, steps) for steps in (1, 2, -1)]
    two = lax.switch(up, forward, after(two, quads))
    current = jnp.stack([one, still, two])
    following = from_ahead(current, 1)
    mine = jnp.concatenate([quads] + [after(piece, two) for piece in got])
    other = fetch(mine, lambda at, core: (at, 1 - core))

    joined = jnp.concatenate([current, following], axis=2)
    slid = jnp.stack(
        [
            lax.dynamic_slice(joined[i], (zero, remainder[i]), basis_series.shape[1:]).T
            for i in range(DETS)
        ]
    )
    shape = (places,) + mine.shape[2:]
    peaks = window_peaks(plan, slid, mine.reshape(shape), other.reshape(shape))
    return lax.switch(middle, home, peaks)


def solution(mesh):
    in_specs = (
        P(None, None, ("groups", "tmpl", "det")),
        P(None, ("groups", "tmpl"), None, None),
        P("groups"),
    )
    out_specs = P(None, ("groups", "tmpl", "det"))
    return jax.shard_map(
        per_device, mesh=mesh, in_specs=in_specs, out_specs=out_specs, check_vma=False
    )
```

```python
import functools
import math

import jax
import jax.numpy as jnp
from jax import lax
from jax.experimental import pallas as pl
from jax.experimental.pallas import tpu as pltpu
from jax.sharding import PartitionSpec as P


DETS = 3
WIN = 128
SLIDES = 16
ROW = 8
FAN = 4
ROW_TILE = 128
BOTH = ("tmpl", "det")


def fetch(value, source_of):
    dets = lax.axis_size("det")
    pairs = []
    for place in range(lax.axis_size("tmpl")):
        for det in range(dets):
            source, source_det = source_of(place, det)
            pairs.append((source * dets + source_det, place * dets + det))
    return lax.ppermute(value, BOTH, pairs)


def from_ahead(value, steps):
    if steps == 0:
        return value
    count = lax.axis_size("tmpl") * lax.axis_size("det")
    return lax.ppermute(value, BOTH, [((i + steps) % count, i) for i in range(count)])


def after(value, *others):
    return lax.optimization_barrier((value, *others))[0]


def fetch_z(value, steps):
    places = lax.axis_size("tmpl")
    row = math.gcd(places, ROW)
    return fetch(value, lambda at, det: ((at + (1 - 2 * det) * steps * row) % places, det))


def plan_kernel(block_len, offsets_ref, plan_ref):
    moved = [lax.div(offsets_ref[i], block_len) for i in range(DETS)]
    ranks = []
    for i in range(DETS):
        rank = jnp.int32(0)
        for j in range(DETS):
            if i != j:
                less = moved[j] <= moved[i] if j < i else moved[j] < moved[i]
                rank = rank + jnp.where(less, 1, 0)
        ranks.append(rank)
    by_rank = []
    for place in range(DETS):
        index, blocks, rest = jnp.int32(0), moved[0], offsets_ref[0]
        for i in range(1, DETS):
            index = jnp.where(ranks[i] == place, i, index)
            blocks = jnp.where(ranks[i] == place, moved[i], blocks)
            rest = jnp.where(ranks[i] == place, offsets_ref[i], rest)
        plan_ref[place] = index
        plan_ref[DETS + place] = lax.rem(rest, block_len)
        by_rank.append(blocks)
    plan_ref[2 * DETS] = by_rank[1] - by_rank[0]
    plan_ref[2 * DETS + 1] = by_rank[2] - by_rank[1]
    plan_ref[2 * DETS + 2] = by_rank[1] - 1


def plan_of(offsets, block_len):
    return pl.pallas_call(
        functools.partial(plan_kernel, block_len),
        in_specs=[pl.BlockSpec(memory_space=pltpu.SMEM)],
        out_specs=pl.BlockSpec(memory_space=pltpu.SMEM),
        out_shape=jax.ShapeDtypeStruct((3 * DETS,), jnp.int32),
        name="plan",
    )(offsets)


def reversed_bits(steps, count):
    slot, bit = jnp.int32(0), 1
    while bit < count:
        slot = slot + lax.rem(lax.div(steps, bit), 2) * (count // 2 // bit)
        bit *= 2
    return slot


def slot_of(steps, rows):
    short = lax.rem(steps, FAN)
    quads = lax.rem(lax.div(steps + lax.div(short, FAN - 1), FAN), rows // FAN)
    return short * (rows // FAN) + quads


def peaks_kernel(plan_ref, slid_ref, mine_ref, other_ref, out_ref, power_ref):
    row = ROW_TILE // mine_ref.shape[2]
    rows = mine_ref.shape[0] // row
    half = row * mine_ref.shape[2]
    place, down = lax.axis_index("tmpl"), lax.axis_index("det")
    z0, x0 = lax.div(place, row), lax.rem(place, row)
    x_slots = [reversed_bits(lax.rem(x - x0 + row, row), row) for x in range(row)]

    def tile(z, _):
        slots = []
        for behind in range(2):
            away = lax.rem(z - z0 - behind + 2 * rows, rows)
            looked_up = slot_of(away, rows) * row
            looked_down = slot_of(lax.rem(rows - away, rows), rows) * row
            slots.append(
                (
                    jnp.where(down == 0, looked_up, looked_down),
                    jnp.where(down == 0, looked_down, looked_up),
                )
            )
        for detector in range(DETS):
            pieces = []
            for side, ref in enumerate((mine_ref, other_ref)):
                for x in range(row):
                    slot = jnp.where(x < x0, slots[1][side], slots[0][side]) + x_slots[x]
                    pieces.append(ref[slot, plan_ref[detector]])
            bank = jnp.concatenate(pieces, axis=0)
            filtered = lax.dot_general(
                slid_ref[detector], bank, (((1,), (1,)), ((), ())),
                preferred_element_type=jnp.float32,
            )
            squared = filtered * filtered
            added = squared[:, :half] + squared[:, half:]
            if detector == 0:
                power_ref[...] = added
            elif detector < DETS - 1:
                power_ref[...] += added
            else:
                power = power_ref[...] + added
                windows = power.shape[0] // WIN
                peak = jnp.max(power.reshape(windows, WIN, half), axis=1)
                out_ref[:, pl.ds(pl.multiple_of(z * half, half), half)] = peak
        return 0

    lax.fori_loop(0, rows, tile, 0, unroll=2)


def window_peaks(plan, slid, mine, other):
    block_len = slid.shape[1]
    templates = mine.shape[0] * mine.shape[2]
    whole = pl.BlockSpec(memory_space=pltpu.VMEM)
    return pl.pallas_call(
        peaks_kernel,
        in_specs=[pl.BlockSpec(memory_space=pltpu.SMEM)] + [whole] * 3,
        out_specs=whole,
        scratch_shapes=[pltpu.VMEM((block_len, ROW_TILE), jnp.float32)],
        out_shape=jax.ShapeDtypeStruct((block_len // WIN, templates), jnp.float32),
        cost_estimate=pl.CostEstimate(
            flops=2 * 2 * DETS * templates * block_len * slid.shape[2],
            bytes_accessed=2 * (slid.size + 2 * mine.size),
            transcendentals=0,
        ),
        name="peaks",
    )(plan, slid, mine, other)


def per_device(basis_series, reconstruction, offsets):
    block_len = basis_series.shape[2]
    places = lax.axis_size("tmpl")
    dets = lax.axis_size("det")
    row = math.gcd(places, ROW)
    rows = places // row
    det = lax.axis_index("det")

    plan = plan_of(offsets, block_len)
    order = plan[:DETS].astype(jnp.uint32)
    remainder = plan[DETS : 2 * DETS].astype(jnp.uint32)
    down, up, middle = (plan[2 * DETS + i] for i in range(3))

    def gather_row(part):
        held, steps = part[None], row // 2
        while steps:
            got = from_ahead(held, steps * dets)
            held = jnp.concatenate([held, got])
            steps //= 2
        return held

    def first_slide(value, part, steps):
        moved = from_ahead(value, -steps)
        return moved, gather_row(part)

    backward = [functools.partial(first_slide, steps=steps) for steps in range(SLIDES - 1)]
    forward = [functools.partial(from_ahead, steps=steps) for steps in range(SLIDES - 1)]
    home = [
        lambda value, steps=steps: from_ahead(value, steps).T for steps in range(1, SLIDES)
    ]

    zero = jnp.uint32(0)
    one, still, two = (
        lax.dynamic_slice(basis_series, (order[i], zero, zero), (1,) + basis_series.shape[1:])[0]
        for i in range(DETS)
    )
    part = lax.dynamic_index_in_dim(reconstruction, det, 2, keepdims=False)
    one, held = lax.switch(down, backward, one, part)

    got = [fetch_z(held, steps) for steps in range(FAN, rows, FAN)]
    two = lax.switch(up, forward, after(two, held))
    quads = jnp.stack([held] + [after(piece, two) for piece in got])

    got = [fetch_z(quads, steps) for steps in (1, 2, -1)]
    current = jnp.stack([one, still, two])
    following = from_ahead(after(current, quads), 1)
    mine = jnp.concatenate([quads] + got)
    other = fetch(mine, lambda at, core: (at, 1 - core))

    joined = jnp.concatenate([current, following], axis=2)
    slid = jnp.stack(
        [
            lax.dynamic_slice(joined[i], (zero, remainder[i]), basis_series.shape[1:]).T
            for i in range(DETS)
        ]
    )
    shape = (places,) + mine.shape[2:]
    powers = window_peaks(plan, slid, mine.reshape(shape), other.reshape(shape))
    return jnp.sqrt(lax.switch(middle, home, powers))


def solution(mesh):
    in_specs = (
        P(None, None, ("groups", "tmpl", "det")),
        P(None, ("groups", "tmpl"), None, None),
        P("groups"),
    )
    out_specs = P(None, ("groups", "tmpl", "det"))
    return jax.shard_map(
        per_device, mesh=mesh, in_specs=in_specs, out_specs=out_specs, check_vma=False
    )
```

```python
import functools
import math

import jax
import jax.numpy as jnp
from jax import lax
from jax.experimental import pallas as pl
from jax.experimental.pallas import tpu as pltpu
from jax.sharding import PartitionSpec as P


DETS = 3
WIN = 128
SLIDES = 16
ROW = 8
FAN = 4
ROW_TILE = 128
BOTH = ("tmpl", "det")


def fetch(value, source_of):
    dets = lax.axis_size("det")
    pairs = []
    for place in range(lax.axis_size("tmpl")):
        for det in range(dets):
            source, source_det = source_of(place, det)
            pairs.append((source * dets + source_det, place * dets + det))
    return lax.ppermute(value, BOTH, pairs)


def from_ahead(value, steps):
    if steps == 0:
        return value
    count = lax.axis_size("tmpl") * lax.axis_size("det")
    return lax.ppermute(value, BOTH, [((i + steps) % count, i) for i in range(count)])


def after(value, *others):
    return lax.optimization_barrier((value, *others))[0]


def fetch_z(value, steps):
    places = lax.axis_size("tmpl")
    row = math.gcd(places, ROW)
    return fetch(value, lambda at, det: ((at + (1 - 2 * det) * steps * row) % places, det))


def plan_kernel(offsets_ref, series_ref, plan_ref, *refs):
    move_refs, sorted_refs, copied = refs[:DETS], refs[DETS : 2 * DETS], refs[-1]
    block_len = series_ref.shape[2]
    moved = [lax.div(offsets_ref[i], block_len) for i in range(DETS)]
    ranks = []
    for i in range(DETS):
        rank = jnp.int32(0)
        for j in range(DETS):
            if i != j:
                less = moved[j] <= moved[i] if j < i else moved[j] < moved[i]
                rank = rank + jnp.where(less, 1, 0)
        ranks.append(rank)
    by_rank, copies = [], []
    for place in range(DETS):
        index, blocks, rest = jnp.int32(0), moved[0], offsets_ref[0]
        for i in range(1, DETS):
            index = jnp.where(ranks[i] == place, i, index)
            blocks = jnp.where(ranks[i] == place, moved[i], blocks)
            rest = jnp.where(ranks[i] == place, offsets_ref[i], rest)
        copies.append(
            pltpu.make_async_copy(series_ref.at[index], sorted_refs[place], copied.at[place])
        )
        copies[-1].start()
        plan_ref[place] = index
        plan_ref[DETS + place] = lax.rem(rest, block_len)
        by_rank.append(blocks)
    move_refs[0][0] = by_rank[1] - by_rank[0]
    move_refs[1][0] = by_rank[2] - by_rank[1]
    move_refs[2][0] = by_rank[1] - 1
    for copy in copies:
        copy.wait()


def plan_of(offsets, series):
    smem, vmem = (pl.BlockSpec(memory_space=space) for space in (pltpu.SMEM, pltpu.VMEM))
    out = pl.pallas_call(
        plan_kernel,
        in_specs=[smem, pl.BlockSpec(memory_space=pltpu.HBM)],
        out_specs=[smem] * (1 + DETS) + [vmem] * DETS,
        out_shape=[jax.ShapeDtypeStruct((2 * DETS,), jnp.int32)]
        + [jax.ShapeDtypeStruct((1,), jnp.int32)] * DETS
        + [jax.ShapeDtypeStruct(series.shape[1:], series.dtype)] * DETS,
        scratch_shapes=[pltpu.SemaphoreType.DMA((DETS,))],
        compiler_params=pltpu.CompilerParams(vmem_limit_bytes=4 << 20),
        name="plan",
    )(offsets, series)
    return out[0], [move[0] for move in out[1 : 1 + DETS]], out[1 + DETS :]


def slot_of(steps, rows):
    short = lax.rem(steps, FAN)
    quads = lax.rem(lax.div(steps + lax.div(short, FAN - 1), FAN), rows // FAN)
    return short * (rows // FAN) + quads


def peaks_kernel(plan_ref, slid_ref, mine_ref, other_ref, out_ref, power_ref):
    row = ROW_TILE // mine_ref.shape[2]
    rows = mine_ref.shape[0] // row
    half = row * mine_ref.shape[2]
    place, down = lax.axis_index("tmpl"), lax.axis_index("det")
    z0, x0 = lax.div(place, row), lax.rem(place, row)
    x_slots = [lax.rem(x - x0 + row, row) for x in range(row)]

    def tile(z, _):
        slots = []
        for behind in range(2):
            away = lax.rem(z - z0 - behind + 2 * rows, rows)
            looked_up = slot_of(away, rows) * row
            looked_down = slot_of(lax.rem(rows - away, rows), rows) * row
            slots.append(
                (
                    jnp.where(down == 0, looked_up, looked_down),
                    jnp.where(down == 0, looked_down, looked_up),
                )
            )
        for detector in range(DETS):
            pieces = []
            for side, ref in enumerate((mine_ref, other_ref)):
                for x in range(row):
                    slot = jnp.where(x < x0, slots[1][side], slots[0][side]) + x_slots[x]
                    pieces.append(ref[slot, plan_ref[detector]])
            bank = jnp.concatenate(pieces, axis=0)
            filtered = lax.dot_general(
                slid_ref[detector], bank, (((1,), (1,)), ((), ())),
                preferred_element_type=jnp.float32,
            )
            squared = filtered * filtered
            added = squared[:, :half] + squared[:, half:]
            if detector == 0:
                power_ref[...] = added
            elif detector < DETS - 1:
                power_ref[...] += added
            else:
                power = power_ref[...] + added
                windows = power.shape[0] // WIN
                peak = jnp.max(power.reshape(windows, WIN, half), axis=1)
                out_ref[:, pl.ds(pl.multiple_of(z * half, half), half)] = peak
        return 0

    lax.fori_loop(0, rows, tile, 0, unroll=2)


def window_peaks(plan, slid, mine, other):
    block_len = slid.shape[1]
    templates = mine.shape[0] * mine.shape[2]
    whole = pl.BlockSpec(memory_space=pltpu.VMEM)
    return pl.pallas_call(
        peaks_kernel,
        in_specs=[pl.BlockSpec(memory_space=pltpu.SMEM)] + [whole] * 3,
        out_specs=whole,
        scratch_shapes=[pltpu.VMEM((block_len, ROW_TILE), jnp.float32)],
        out_shape=jax.ShapeDtypeStruct((block_len // WIN, templates), jnp.float32),
        cost_estimate=pl.CostEstimate(
            flops=2 * 2 * DETS * templates * block_len * slid.shape[2],
            bytes_accessed=2 * (slid.size + 2 * mine.size),
            transcendentals=0,
        ),
        compiler_params=pltpu.CompilerParams(vmem_limit_bytes=16 << 20),
        name="peaks",
    )(plan, slid, mine, other)


def per_device(basis_series, reconstruction, offsets):
    places = lax.axis_size("tmpl")
    dets = lax.axis_size("det")
    row = math.gcd(places, ROW)
    rows = places // row
    det = lax.axis_index("det")

    plan, (down, up, middle), (one, still, two) = plan_of(offsets, basis_series)
    remainder = plan[DETS:].astype(jnp.uint32)

    def gather_row(part):
        held, steps = part[None], 1
        while steps < row:
            got = from_ahead(held, steps * dets)
            held = jnp.concatenate([held, got])
            steps *= 2
        return held

    def first_slide(value, part, steps):
        moved = from_ahead(value, -steps)
        return moved, gather_row(part)

    backward = [functools.partial(first_slide, steps=steps) for steps in range(SLIDES - 1)]
    forward = [functools.partial(from_ahead, steps=steps) for steps in range(SLIDES - 1)]
    home = [
        lambda value, steps=steps: from_ahead(value, steps).T for steps in range(1, SLIDES)
    ]

    part = lax.dynamic_index_in_dim(reconstruction, det, 2, keepdims=False)
    one, held = lax.switch(down, backward, one, part)

    got = [fetch_z(held, steps) for steps in range(FAN, rows, FAN)]
    two = lax.switch(up, forward, after(two, held))
    quads = jnp.stack([held] + [after(piece, two) for piece in got])

    current = jnp.stack([one, still, two])
    following = from_ahead(after(current, quads), 1)
    got = [fetch_z(quads, steps) for steps in (1, 2, -1)]

    joined = jnp.concatenate([current, following], axis=2)
    slid = jnp.stack(
        [
            lax.dynamic_slice(joined[i], (jnp.uint32(0), remainder[i]), one.shape).T
            for i in range(DETS)
        ]
    )
    mine = jnp.concatenate([quads] + [after(piece, slid) for piece in got])
    other = fetch(mine, lambda at, core: (at, 1 - core))
    shape = (places,) + mine.shape[2:]
    powers = window_peaks(plan, slid, mine.reshape(shape), other.reshape(shape))
    return jnp.sqrt(lax.switch(middle, home, powers))


def solution(mesh):
    in_specs = (
        P(None, None, ("groups", "tmpl", "det")),
        P(None, ("groups", "tmpl"), None, None),
        P("groups"),
    )
    out_specs = P(None, ("groups", "tmpl", "det"))
    return jax.shard_map(
        per_device, mesh=mesh, in_specs=in_specs, out_specs=out_specs, check_vma=False
    )
```

```python
import functools
import math

import jax
import jax.numpy as jnp
from jax import lax
from jax.experimental import pallas as pl
from jax.experimental.pallas import tpu as pltpu
from jax.sharding import PartitionSpec as P


DETS = 3
WIN = 128
SLIDES = 16
ROW = 8
FAN = 4
ROW_TILE = 128
BOTH = ("tmpl", "det")


def fetch(value, source_of):
    dets = lax.axis_size("det")
    pairs = []
    for place in range(lax.axis_size("tmpl")):
        for det in range(dets):
            source, source_det = source_of(place, det)
            pairs.append((source * dets + source_det, place * dets + det))
    return lax.ppermute(value, BOTH, pairs)


def from_ahead(value, steps):
    if steps == 0:
        return value
    count = lax.axis_size("tmpl") * lax.axis_size("det")
    return lax.ppermute(value, BOTH, [((i + steps) % count, i) for i in range(count)])


def after(value, *others):
    return lax.optimization_barrier((value, *others))[0]


def fetch_z(value, steps):
    places = lax.axis_size("tmpl")
    row = math.gcd(places, ROW)
    return fetch(value, lambda at, det: ((at + (1 - 2 * det) * steps * row) % places, det))


def plan_kernel(offsets_ref, series_ref, plan_ref, *refs):
    move_refs, sorted_refs, copied = refs[:DETS], refs[DETS : 2 * DETS], refs[-1]
    block_len = series_ref.shape[2]
    moved = [lax.div(offsets_ref[i], block_len) for i in range(DETS)]
    ranks = []
    for i in range(DETS):
        rank = jnp.int32(0)
        for j in range(DETS):
            if i != j:
                less = moved[j] <= moved[i] if j < i else moved[j] < moved[i]
                rank = rank + jnp.where(less, 1, 0)
        ranks.append(rank)
    by_rank, copies = [], []
    for place in range(DETS):
        index, blocks, rest = jnp.int32(0), moved[0], offsets_ref[0]
        for i in range(1, DETS):
            index = jnp.where(ranks[i] == place, i, index)
            blocks = jnp.where(ranks[i] == place, moved[i], blocks)
            rest = jnp.where(ranks[i] == place, offsets_ref[i], rest)
        copies.append(
            pltpu.make_async_copy(series_ref.at[index], sorted_refs[place], copied.at[place])
        )
        copies[-1].start()
        plan_ref[place] = index
        plan_ref[DETS + place] = lax.rem(rest, block_len)
        by_rank.append(blocks)
    move_refs[0][0] = by_rank[1] - by_rank[0]
    move_refs[1][0] = by_rank[2] - by_rank[1]
    move_refs[2][0] = by_rank[1] - 1
    for copy in copies:
        copy.wait()


def plan_of(offsets, series):
    smem, vmem = (pl.BlockSpec(memory_space=space) for space in (pltpu.SMEM, pltpu.VMEM))
    out = pl.pallas_call(
        plan_kernel,
        in_specs=[smem, pl.BlockSpec(memory_space=pltpu.HBM)],
        out_specs=[smem] * (1 + DETS) + [vmem] * DETS,
        out_shape=[jax.ShapeDtypeStruct((2 * DETS,), jnp.int32)]
        + [jax.ShapeDtypeStruct((1,), jnp.int32)] * DETS
        + [jax.ShapeDtypeStruct(series.shape[1:], series.dtype)] * DETS,
        scratch_shapes=[pltpu.SemaphoreType.DMA((DETS,))],
        compiler_params=pltpu.CompilerParams(vmem_limit_bytes=4 << 20),
        name="plan",
    )(offsets, series)
    return out[0], [move[0] for move in out[1 : 1 + DETS]], out[1 + DETS :]


def reversed_bits(steps, count):
    slot, bit = jnp.int32(0), 1
    while bit < count:
        slot = slot + lax.rem(lax.div(steps, bit), 2) * (count // 2 // bit)
        bit *= 2
    return slot


def slot_of(steps, rows):
    short = lax.rem(steps, FAN)
    quads = lax.rem(lax.div(steps + lax.div(short, FAN - 1), FAN), rows // FAN)
    return short * (rows // FAN) + quads


def peaks_kernel(plan_ref, slid_ref, mine_ref, other_ref, out_ref, power_ref):
    row = ROW_TILE // mine_ref.shape[2]
    rows = mine_ref.shape[0] // row
    half = row * mine_ref.shape[2]
    place, down = lax.axis_index("tmpl"), lax.axis_index("det")
    z0, x0 = lax.div(place, row), lax.rem(place, row)
    x_slots = [reversed_bits(lax.rem(x - x0 + row, row), row) for x in range(row)]

    def tile(z, _):
        slots = []
        for behind in range(2):
            away = lax.rem(z - z0 - behind + 2 * rows, rows)
            looked_up = slot_of(away, rows) * row
            looked_down = slot_of(lax.rem(rows - away, rows), rows) * row
            slots.append(
                (
                    jnp.where(down == 0, looked_up, looked_down),
                    jnp.where(down == 0, looked_down, looked_up),
                )
            )
        for detector in range(DETS):
            pieces = []
            for side, ref in enumerate((mine_ref, other_ref)):
                for x in range(row):
                    slot = jnp.where(x < x0, slots[1][side], slots[0][side]) + x_slots[x]
                    pieces.append(ref[slot, plan_ref[detector]])
            bank = jnp.concatenate(pieces, axis=0)
            filtered = lax.dot_general(
                slid_ref[detector], bank, (((1,), (1,)), ((), ())),
                preferred_element_type=jnp.float32,
            )
            squared = filtered * filtered
            added = squared[:, :half] + squared[:, half:]
            if detector == 0:
                power_ref[...] = added
            elif detector < DETS - 1:
                power_ref[...] += added
            else:
                power = power_ref[...] + added
                windows = power.shape[0] // WIN
                peak = jnp.max(power.reshape(windows, WIN, half), axis=1)
                out_ref[:, pl.ds(pl.multiple_of(z * half, half), half)] = peak
        return 0

    lax.fori_loop(0, rows, tile, 0, unroll=2)


def window_peaks(plan, slid, mine, other):
    block_len = slid.shape[1]
    templates = mine.shape[0] * mine.shape[2]
    whole = pl.BlockSpec(memory_space=pltpu.VMEM)
    return pl.pallas_call(
        peaks_kernel,
        in_specs=[pl.BlockSpec(memory_space=pltpu.SMEM)] + [whole] * 3,
        out_specs=whole,
        scratch_shapes=[pltpu.VMEM((block_len, ROW_TILE), jnp.float32)],
        out_shape=jax.ShapeDtypeStruct((block_len // WIN, templates), jnp.float32),
        cost_estimate=pl.CostEstimate(
            flops=2 * 2 * DETS * templates * block_len * slid.shape[2],
            bytes_accessed=2 * (slid.size + 2 * mine.size),
            transcendentals=0,
        ),
        compiler_params=pltpu.CompilerParams(vmem_limit_bytes=16 << 20),
        name="peaks",
    )(plan, slid, mine, other)


def per_device(basis_series, reconstruction, offsets):
    places = lax.axis_size("tmpl")
    dets = lax.axis_size("det")
    row = math.gcd(places, ROW)
    rows = places // row
    det = lax.axis_index("det")

    plan, (down, up, middle), (one, still, two) = plan_of(offsets, basis_series)
    remainder = plan[DETS:].astype(jnp.uint32)

    def gather_row(part):
        held, steps = part[None], row // 2
        while steps:
            got = from_ahead(held, steps * dets)
            held = jnp.concatenate([held, got])
            steps //= 2
        return held

    def first_slide(value, part, steps):
        moved = from_ahead(value, -steps)
        return moved, gather_row(part)

    backward = [functools.partial(first_slide, steps=steps) for steps in range(SLIDES - 1)]
    forward = [functools.partial(from_ahead, steps=steps) for steps in range(SLIDES - 1)]
    home = [
        lambda value, steps=steps: from_ahead(value, steps).T for steps in range(1, SLIDES)
    ]

    part = lax.dynamic_index_in_dim(reconstruction, det, 2, keepdims=False)
    one, held = lax.switch(down, backward, one, part)

    got = [fetch_z(held, steps) for steps in range(FAN, rows, FAN)]
    two = lax.switch(up, forward, after(two, held))
    quads = jnp.stack([held] + [after(piece, two) for piece in got])

    got = [fetch_z(quads, steps) for steps in (1, 2, -1)]
    current = jnp.stack([one, still, two])
    following = from_ahead(after(current, quads), 1)
    mine = jnp.concatenate([quads] + got)
    other = fetch(mine, lambda at, core: (at, 1 - core))

    joined = jnp.concatenate([current, following], axis=2)
    slid = jnp.stack(
        [
            lax.dynamic_slice(joined[i], (jnp.uint32(0), remainder[i]), one.shape).T
            for i in range(DETS)
        ]
    )
    shape = (places,) + mine.shape[2:]
    powers = window_peaks(plan, slid, mine.reshape(shape), other.reshape(shape))
    return jnp.sqrt(lax.switch(middle, home, powers))


def solution(mesh):
    in_specs = (
        P(None, None, ("groups", "tmpl", "det")),
        P(None, ("groups", "tmpl"), None, None),
        P("groups"),
    )
    out_specs = P(None, ("groups", "tmpl", "det"))
    return jax.shard_map(
        per_device, mesh=mesh, in_specs=in_specs, out_specs=out_specs, check_vma=False
    )
```
